32 devices in a mesh: rep: 2 (over y), gx: 8 (over z, x), gy: 2 (over core).
Axes of the slice: x: 2, y: 2, z: 4, core: 2. Of those that a mesh axis runs over, the one named last changes fastest.
Arguments:
- tokens: bfloat16 [768, 8192], P(('rep', 'gx'), 'gy'), parts along dimension 0, may hold values from -6 to 6
- segment_ids: int32 [768], P(('rep', 'gx')), parts along dimension 0, may hold values from 0 to 1, as said below
- gate_weight: bfloat16 [8192, 2, 13312], P(None, 'gy', 'gx'), may hold values from -0.0625 to 0.0625
- up_weight: bfloat16 [8192, 2, 13312], P(None, 'gy', 'gx'), may hold values from -0.0625 to 0.0625
- down_weight: bfloat16 [2, 13312, 8192], P('gy', None, 'gx'), may hold values from -0.0390625 to 0.0390625
Outputs:
- grouped: bfloat16 [768, 8192], P(('rep', 'gx'), 'gy'), parts along dimension 0
The draws below stay inside these ranges and needn't reach their ends.
There are 2 independent parts, one for each index of `rep`. The reference program is written for one: setup_inputs(seed, part) draws one part's arguments, and reference() takes and returns one part's arrays. A program takes and returns all parts, laid end to end along the dimension named above; an argument that names none is the same for every part. Nothing has to cross between parts.
Inputs may be any that keep to these rules, and one draw needn't show every extreme that they name: `segment_ids`: exactly 320 entries are 0 and 64 entries are 1.
All inputs are finite; a program needn't handle non-finite values.
Results may differ from the reference program's by a relative error of at most 0.0049.
Values may be sent and summed in bfloat16 or wider, within the bound.
A program may use at most 128 MiB of HBM per device.

```python
import jax
import jax.numpy as jnp

D = 8192
FF = 26624
PREFILL = 320
DECODE = 64
TOKENS = 384


def draw_segment_ids(key, part):
    shuffled = jax.random.permutation(key, PREFILL + DECODE)
    return (shuffled >= PREFILL).astype(jnp.int32)


def steps_of(own_key, shape, pieces, low, top_value):
    loudness = 1.0
    for axis_at, shards_of in pieces:
        draws = jax.random.uniform(jax.random.fold_in(jax.random.fold_in(own_key, 6), axis_at), (shards_of,), jnp.float32, low / len(pieces), top_value / len(pieces))
        loudness = loudness * jnp.repeat(jnp.exp(draws), shape[axis_at] // shards_of).reshape((-1,) + (1,) * (len(shape) - 1 - axis_at))
    return loudness


def noise(rng, shape, spread, bound, cuts=(), dtype=jnp.bfloat16):
    result = spread * jax.random.normal(rng, shape, jnp.float32)
    if cuts:
        result = result * steps_of(rng, shape, cuts, -0.22, 0.18)
    return jnp.clip(result, -bound, bound).astype(dtype)


def setup_inputs(seed: int = 0, part: int = 0) -> dict:
    key_list = jax.random.split(jax.random.key(seed), 6)
    own_keys = jax.random.split(jax.random.fold_in(key_list[5], part), 6)
    return {
        "tokens": noise(own_keys[0], (TOKENS, D), 1.0, 6.0, ((0, 8), (1, 2))),
        "segment_ids": draw_segment_ids(jax.random.fold_in(jax.random.fold_in(key_list[5], part), 71), part),
        "gate_weight": noise(key_list[2], (D, 2, FF // 2), D ** -0.5, 0.0625, ((1, 2), (2, 8))),
        "up_weight": noise(key_list[3], (D, 2, FF // 2), D ** -0.5, 0.0625, ((1, 2), (2, 8))),
        "down_weight": noise(key_list[4], (2, FF // 2, D), FF ** -0.5, 0.0390625, ((0, 2), (2, 8))),
    }


def grouped_target(segment_ids):
    decode_flag = segment_ids.astype(jnp.int32)
    prefill_flag = 1 - decode_flag
    prefill_rank = (jnp.cumsum(prefill_flag) - 1).astype(jnp.int32)
    decode_rank = (jnp.cumsum(decode_flag) - 1).astype(jnp.int32)
    return jnp.where(decode_flag == 0, prefill_rank, PREFILL + decode_rank).astype(jnp.int32)


def reference(tokens, segment_ids, gate_weight, up_weight, down_weight):
    gate_matrix = gate_weight.reshape(D, FF)
    up_matrix = up_weight.reshape(D, FF)
    down_matrix = down_weight.reshape(FF, D)
    gate_value = jnp.dot(tokens, gate_matrix, preferred_element_type=jnp.float32)
    up_value = jnp.dot(tokens, up_matrix, preferred_element_type=jnp.float32)
    hidden = (jax.nn.silu(gate_value) * up_value).astype(jnp.bfloat16)
    product = jnp.dot(hidden, down_matrix, preferred_element_type=jnp.float32)
    target = grouped_target(segment_ids)
    placed = jnp.zeros_like(product).at[target].set(product)
    return placed.astype(jnp.bfloat16)
```

```python
import functools

import jax
import jax.numpy as jnp
from jax import lax
from jax.experimental import pallas as pl
from jax.experimental.pallas import tpu as pltpu
from jax.sharding import PartitionSpec as P

PREFILL = 320
MESH = pl.DeviceIdType.MESH
LANES = 128
W_SLOTS = 3
TOKEN_MESSAGES = 4
LAG1, LAG2, LAG3 = 2, 4, 6


def grouped_target(token_kinds):
    decode_flag = token_kinds.astype(jnp.int32)
    prefill_flag = 1 - decode_flag
    prefill_rank = jnp.cumsum(prefill_flag) - 1
    decode_rank = jnp.cumsum(decode_flag) - 1
    return jnp.where(decode_flag == 0, prefill_rank, PREFILL + decode_rank)


def plain(tokens, segment_ids, gate_weight, up_weight, down_weight):
    half_rows, token_kinds = (
        lax.all_gather(tokens, "gx", axis=0, tiled=True),
        lax.all_gather(segment_ids, "gx", axis=0, tiled=True),
    )
    gathered = lax.all_gather(half_rows, "gy", axis=1, tiled=True)
    gate_local = gate_weight.reshape(gate_weight.shape[0], -1)
    up_local = up_weight.reshape(up_weight.shape[0], -1)
    down_local = down_weight.reshape(-1, down_weight.shape[2])
    target = grouped_target(token_kinds)
    gate_value = jnp.dot(gathered, gate_local, preferred_element_type=jnp.float32)
    up_value = jnp.dot(gathered, up_local, preferred_element_type=jnp.float32)
    hidden = (jax.nn.silu(gate_value) * up_value).astype(jnp.bfloat16)
    partial_value = jnp.dot(
        lax.all_gather(hidden, "gx", axis=1, tiled=True),
        down_local,
        preferred_element_type=jnp.float32,
    )
    placed = jnp.zeros_like(partial_value).at[target].set(partial_value)
    switched = lax.all_to_all(placed, "gx", split_axis=0, concat_axis=1, tiled=True)
    return lax.psum_scatter(switched, "gy", scatter_dimension=1, tiled=True).astype(jnp.bfloat16)


def kernel(
    n, tokens, kinds, gate, up, down, out,
    x, w, d, h, acc, other, kinds_all, place, stage, landed,
    own_sem, w_sem, d_sem, kind_send, kind_recv,
    t_send, t_recv, p_send, p_recv, h_send, h_recv,
    a_send, a_recv, o_send, o_recv, o_local,
):
    rows, half = tokens.shape
    total_rows = n * rows
    chunks = h.shape[0]
    local_units = chunks * LANES
    rep, me, core = lax.axis_index("rep"), lax.axis_index("gx"), lax.axis_index("gy")
    peer = 1 - core

    def flip(g):
        return g + 1 - 2 * lax.rem(g, 2)

    xn = flip(me)
    zp = lax.rem(me + 2, n)
    zm = lax.rem(me + n - 2, n)
    far = lax.rem(me + n // 2, n)

    def w_load(c):
        b = lax.rem(c, W_SLOTS)
        cols = pl.ds(pl.multiple_of(c * LANES, LANES), LANES)
        return [
            pltpu.make_async_copy(ref.at[:, cols], w.at[b, :, pl.ds(i * LANES, LANES)], w_sem.at[b, i])
            for i, ref in enumerate((gate, up))
        ]

    own_rows = pl.ds(pl.multiple_of(me * rows, rows), rows)
    own_cols = pl.ds(pl.multiple_of(core * half, half), half)
    own_copy = pltpu.make_async_copy(tokens, x.at[own_rows, own_cols], own_sem)
    own_copy.start()
    for c in range(W_SLOTS):
        for copy in w_load(c):
            copy.start()

    barrier = pltpu.get_barrier_semaphore()
    for step in range(n):
        for k in range(2):
            if step == 0 and k == 0:
                continue
            pl.semaphore_signal(
                barrier, inc=1,
                device_id=(rep, lax.rem(me + step, n), lax.rem(core + k, 2)), device_id_type=MESH,
            )
    pl.semaphore_wait(barrier, 2 * n - 1)

    def remote(src, dst, send, recv, g, k):
        return pltpu.make_async_remote_copy(
            src_ref=src, dst_ref=dst, send_sem=send, recv_sem=recv,
            device_id=(rep, g, k), device_id_type=MESH,
        )

    def regions(message):
        ref = message["region"]
        return [
            (ref, xn, None), (ref, zm, None), (ref, zp, None),
            (ref, far, 0), (ref, far, 1),
            (ref, flip(zm), None), (ref, flip(zp), None),
            (ref, flip(far), 0), (ref, flip(far), 1),
        ]

    def push(message, slot, src_g, part, to):
        ref = message["region"](src_g, part)
        remote(ref, ref, message["send"](slot), message["recv"](slot), to, core).start()

    def take(message, slot):
        fn, g, part = regions(message)[slot]
        ref = fn(g, part)
        remote(ref, ref, message["send"](slot), message["recv"](slot), me, core).wait_recv()
        if message["arrived"] is not None:
            message["arrived"](slot, ref)

    def drain(message):
        for slot, (fn, g, part) in enumerate(regions(message)):
            ref = fn(g, part)
            remote(ref, ref, message["send"](slot), message["recv"](slot), me, core).wait_send()

    def stage0(message, kind):
        push(message, 0, me, None, xn)
        push(message, 1, me, None, zp)
        push(message, 2, me, None, zm)

    def stage1(message, kind):
        if kind == 0:
            take(message, 0)
            push(message, 5, xn, None, zp)
            push(message, 6, xn, None, zm)
        take(message, 1)
        push(message, 3, zm, 0, zp)
        if kind == 1:
            push(message, 5, zm, None, xn)
        take(message, 2)
        push(message, 4, zp, 1, zm)
        if kind == 1:
            push(message, 6, zp, None, xn)

    def stage2(message, kind):
        if kind == 0:
            take(message, 5)
            push(message, 7, flip(zm), 0, zp)
            take(message, 6)
            push(message, 8, flip(zp), 1, zm)
        else:
            take(message, 3)
            push(message, 7, far, 0, xn)
            take(message, 4)
            push(message, 8, far, 1, xn)

    def stage3(message, kind):
        for slot in (3, 4, 7, 8) if kind == 0 else (0, 5, 6, 7, 8):
            take(message, slot)

    width = half // TOKEN_MESSAGES

    def token_message(m):
        def region(g, part):
            start = core * half + m * width
            size = width
            if part is not None:
                size = width // 2
                start = start + part * size
            return x.at[pl.ds(pl.multiple_of(g * rows, rows), rows), pl.ds(pl.multiple_of(start, LANES), size)]

        def arrived(slot, ref):
            remote(ref, ref, p_send.at[m, slot], p_recv.at[m, slot], me, peer).start()

        return dict(
            region=region, arrived=arrived,
            send=lambda s: t_send.at[m, s], recv=lambda s: t_recv.at[m, s],
        )

    messages = [(token_message(m), m % 2) for m in range(TOKEN_MESSAGES)]
    own_copy.wait()
    for message, kind in messages:
        stage0(message, kind)
    own_ref = x.at[own_rows, own_cols]
    own_push = remote(own_ref, own_ref, o_local.at[1], o_local.at[2], me, peer)
    own_push.start()
    kind_copies = []
    for step in range(1, n):
        g = lax.rem(me + step, n)
        copy = remote(kinds, kinds_all.at[n - step], kind_send.at[step], kind_recv.at[n - step], g, core)
        copy.start()
        kind_copies.append(copy)

    def d_start(i, carry):
        c, g = i // n, lax.rem(i, n)
        pltpu.make_async_copy(
            down.at[pl.ds(pl.multiple_of(g * local_units + c * LANES, LANES), LANES), :],
            d.at[c, pl.ds(pl.multiple_of(g * LANES, LANES), LANES), :],
            d_sem.at[c],
        ).start()
        return carry

    lax.fori_loop(0, chunks * n, d_start, 0)

    for run in (stage1, stage2, stage3):
        for message, kind in messages:
            run(message, kind)
    peer_cols = peer * half
    remote(
        own_ref, x.at[own_rows, pl.ds(pl.multiple_of(peer_cols, LANES), half)],
        o_local.at[1], o_local.at[2], me, peer,
    ).wait_recv()
    for m, (message, kind) in enumerate(messages):
        for slot, (fn, g, part) in enumerate(regions(message)):
            start = peer_cols + m * width
            size = width
            if part is not None:
                size = width // 2
                start = start + part * size
            dst = x.at[pl.ds(pl.multiple_of(g * rows, rows), rows), pl.ds(pl.multiple_of(start, LANES), size)]
            remote(dst, dst, p_send.at[m, slot], p_recv.at[m, slot], me, peer).wait_recv()

    def chunk_message(c):
        def region(g, part):
            cols = pl.ds(pl.multiple_of(g * LANES, LANES), LANES)
            if part is None:
                return h.at[c, :, cols]
            size = total_rows // 2
            return h.at[c, pl.ds(part * size, size), cols]

        return dict(
            region=region, arrived=None,
            send=lambda s: h_send.at[c, s], recv=lambda s: h_recv.at[c, s],
        )

    def by_kind(c, fn):
        for kind in range(2):
            @pl.when(lax.rem(c, 2) == kind)
            def _():
                fn(chunk_message(c), kind)

    acc[...] = jnp.zeros_like(acc)

    def step_fn(t, carry):
        @pl.when(t < chunks)
        def _():
            b = lax.rem(t, W_SLOTS)
            for copy in w_load(t):
                copy.wait()
            both = jnp.dot(x[...], w[b], preferred_element_type=jnp.float32)
            gate_value, up_value = both[:, :LANES], both[:, LANES:]
            hidden = gate_value / (1.0 + jnp.exp(-gate_value)) * up_value
            h[t, :, pl.ds(pl.multiple_of(me * LANES, LANES), LANES)] = hidden.astype(jnp.bfloat16)
            stage0(chunk_message(t), 0)

            @pl.when(t + W_SLOTS < chunks)
            def _():
                for copy in w_load(t + W_SLOTS):
                    copy.start()

        @pl.when((t >= LAG1) & (t < chunks + LAG1))
        def _():
            by_kind(t - LAG1, stage1)

        @pl.when((t >= LAG2) & (t < chunks + LAG2))
        def _():
            by_kind(t - LAG2, stage2)

        @pl.when(t >= LAG3)
        def _():
            c = t - LAG3
            by_kind(c, stage3)
            pltpu.make_async_copy(down.at[pl.ds(0, n * LANES), :], d.at[c], d_sem.at[c]).wait()
            cut = acc.shape[2]
            for j in range(2):
                acc[j] += jnp.dot(
                    h[c], d[c, :, j * cut : (j + 1) * cut], preferred_element_type=jnp.float32
                )

        @pl.when(t == chunks)
        def _():
            for i in range(1, n):
                remote(kinds, kinds_all.at[i], kind_send.at[i], kind_recv.at[i], me, core).wait_recv()
            flags = kinds[...]
            for i in range(1, n):
                flags = flags + kinds_all[i]
            flags = flags.astype(jnp.float32)
            shape = (total_rows, total_rows)
            down_iota = lax.broadcasted_iota(jnp.int32, shape, 0)
            lane_iota = lax.broadcasted_iota(jnp.int32, shape, 1)
            upper = jnp.where(down_iota <= lane_iota, 1.0, 0.0).astype(jnp.bfloat16)
            count = jnp.dot(flags.astype(jnp.bfloat16), upper, preferred_element_type=jnp.float32)
            index = lax.broadcasted_iota(jnp.int32, flags.shape, 1).astype(jnp.float32)
            target = jnp.where(flags == 0.0, index - count, PREFILL - 1.0 + count)
            wanted = jnp.broadcast_to(target[0:1, :], shape)
            place[...] = jnp.where(wanted == down_iota.astype(jnp.float32), 1.0, 0.0).astype(jnp.bfloat16)

        return carry

    lax.fori_loop(0, chunks + LAG3, step_fn, 0)

    swap = remote(acc.at[peer], other, a_send, a_recv, me, peer)
    swap.start()
    swap.wait_recv()
    summed = (acc[core] + other[...]).astype(jnp.bfloat16)
    placed = jnp.dot(place[...], summed, preferred_element_type=jnp.float32).astype(jnp.bfloat16)
    cut = acc.shape[2]
    for g in range(n):
        stage[g] = placed[g * rows : (g + 1) * rows]
    quarter = n // 2
    owner_core, position = me // quarter, lax.rem(me, quarter)
    slot = position * 2 + core
    cols = pl.ds(pl.multiple_of(slot * cut, cut), cut)
    for step in range(1, n):
        g = lax.rem(me + step, n)
        remote(stage.at[g], landed.at[:, cols], o_send.at[step], o_recv.at[slot], g, owner_core).start()

    @pl.when(core == owner_core)
    def _():
        copy = pltpu.make_async_copy(stage.at[me], out.at[:, cols], o_local.at[0])
        copy.start()
        copy.wait()

    @pl.when(core != owner_core)
    def _():
        remote(stage.at[me], landed.at[:, cols], o_send.at[0], o_recv.at[slot], me, owner_core).start()

    for s in range(n):
        view = pl.ds(s * cut, cut)
        from_g = core * quarter + s // 2
        mine = (from_g == me) & (core == s % 2)

        @pl.when(jnp.logical_not(mine))
        def _():
            remote(stage.at[0], landed.at[:, view], o_send.at[0], o_recv.at[s], me, core).wait_recv()
            copy = pltpu.make_async_copy(landed.at[:, view], out.at[:, view], o_local.at[0])
            copy.start()
            copy.wait()

    swap.wait_send()
    own_push.wait_send()
    for copy in kind_copies:
        copy.wait_send()
    for m, (message, kind) in enumerate(messages):
        drain(message)
        for s, (fn, g, part) in enumerate(regions(message)):
            ref = fn(g, part)
            remote(ref, ref, p_send.at[m, s], p_recv.at[m, s], me, peer).wait_send()

    def drain_chunk(c, carry):
        drain(chunk_message(c))
        return carry

    lax.fori_loop(0, chunks, drain_chunk, 0)
    for step in range(1, n):
        remote(stage.at[0], landed.at[:, cols], o_send.at[step], o_recv.at[slot], me, core).wait_send()

    @pl.when(core != owner_core)
    def _():
        remote(stage.at[0], landed.at[:, cols], o_send.at[0], o_recv.at[slot], me, core).wait_send()


def fused(n, tokens, segment_ids, gate_weight, up_weight, down_weight):
    rows, half = tokens.shape
    total_rows, width = n * rows, 2 * half
    units = gate_weight.shape[2]
    chunks = units // LANES
    features = down_weight.shape[2]
    me = lax.axis_index("gx")
    kinds = lax.dynamic_update_slice(
        jnp.zeros((8, total_rows), jnp.int32),
        jnp.broadcast_to(segment_ids.astype(jnp.int32)[None], (8, rows)),
        (0, me * rows),
    )
    cut = features // 2
    dma = pltpu.SemaphoreType.DMA
    any_spec = pl.BlockSpec(memory_space=pl.ANY)
    return pl.pallas_call(
        functools.partial(kernel, n),
        out_shape=jax.ShapeDtypeStruct((rows, half), jnp.bfloat16),
        in_specs=[any_spec, pl.BlockSpec(memory_space=pltpu.VMEM), any_spec, any_spec, any_spec],
        out_specs=any_spec,
        scratch_shapes=[
            pltpu.VMEM((total_rows, width), jnp.bfloat16),
            pltpu.VMEM((W_SLOTS, width, 2 * LANES), jnp.bfloat16),
            pltpu.VMEM((chunks, n * LANES, features), jnp.bfloat16),
            pltpu.VMEM((chunks, total_rows, n * LANES), jnp.bfloat16),
            pltpu.VMEM((2, total_rows, cut), jnp.float32),
            pltpu.VMEM((total_rows, cut), jnp.float32),
            pltpu.VMEM((n, 8, total_rows), jnp.int32),
            pltpu.VMEM((total_rows, total_rows), jnp.bfloat16),
            pltpu.VMEM((n, rows, cut), jnp.bfloat16),
            pltpu.VMEM((rows, half), jnp.bfloat16),
            dma, dma((W_SLOTS, 2)), dma((chunks,)), dma((n,)), dma((n,)),
            dma((TOKEN_MESSAGES, 9)), dma((TOKEN_MESSAGES, 9)),
            dma((TOKEN_MESSAGES, 9)), dma((TOKEN_MESSAGES, 9)),
            dma((chunks, 9)), dma((chunks, 9)),
            dma, dma, dma((n,)), dma((n,)), dma((3,)),
        ],
        compiler_params=pltpu.CompilerParams(
            collective_id=0, has_side_effects=True, vmem_limit_bytes=67_043_328
        ),
    )(
        tokens, kinds, gate_weight.reshape(width, units), up_weight.reshape(width, units),
        down_weight.reshape(n * units, features),
    )


def solution(mesh):
    n = mesh.shape["gx"]

    def local(tokens, segment_ids, gate_weight, up_weight, down_weight):
        rows, half = tokens.shape
        features = down_weight.shape[2]
        fits = (
            n == 8
            and mesh.shape["gy"] == 2
            and rows % 16 == 0
            and (n * rows) % LANES == 0
            and gate_weight.shape[2] % LANES == 0
            and half % (2 * LANES * TOKEN_MESSAGES) == 0
            and features % (2 * LANES) == 0
            and features * n == 2 * half
        )
        if fits:
            return fused(n, tokens, segment_ids, gate_weight, up_weight, down_weight)
        return plain(tokens, segment_ids, gate_weight, up_weight, down_weight)

    placed = (
        P(("rep", "gx"), "gy"),
        P(("rep", "gx")),
        P(None, "gy", "gx"),
        P(None, "gy", "gx"),
        P("gy", None, "gx"),
    )
    return jax.shard_map(
        local, mesh=mesh, in_specs=placed, out_specs=P(("rep", "gx"), "gy"), check_vma=False
    )
```
